512 devices in a mesh: pts: 32 (over x, y, core), cand: 16 (over z).
Axes of the slice: x: 4, y: 4, z: 16, core: 2. Of those that a mesh axis runs over, the one named last changes fastest.
Arguments:
- points: bfloat16 [32768, 1024], P('pts'), may hold values from -6 to 6
- weights: float32 [32768], P('pts'), may hold values from 0.5 to 5
- coverage: float32 [32768], P('pts'), may hold values from -0.5 to 1
- candidates: bfloat16 [16384, 1024], P('cand'), may hold values from -6 to 6
- picks: int32 [64], replicated, may hold values from 0 to 16383
Outputs:
- gains: float32 [16384], P('cand')
- top_gains: float32 [64], replicated
- new_coverage: float32 [32768], P('pts')
The draws below stay inside these ranges and needn't reach their ends.
All inputs are finite; a program needn't handle non-finite values.
Results may differ from the reference program's by a relative error of at most 0.0003.
Values may be sent and summed in bfloat16 or wider, within the bound.
No kernel may reach another device: no remote copies, remote signals or barrier semaphores. Data moves between devices by JAX's collectives and lax.ppermute only.
A program may use at most 64 MiB of HBM per device.

```python
import math
import jax
import jax.numpy as jnp
from jax import lax

D = 1024
CAND_DEV = 1024
NPICK = 64
TOPK = 64
NPTS = 32768
NCAND = 16384
N_CAND = 16


def set_ends(result, rng, smallest, top_value):
    dims = result.shape
    place = [jax.random.randint(jax.random.fold_in(rng, axis), (), 0, dims[axis]) for axis in range(len(dims))]
    result = result.at[tuple(place)].set(smallest)
    longest = dims.index(max(dims))
    place[longest] = (place[longest] + 1) % dims[longest]
    return result.at[tuple(place)].set(top_value)


def block_levels(stream_key, dims, shards, smallest, largest):
    def one(position, parts):
        heights = jax.random.uniform(jax.random.fold_in(jax.random.fold_in(stream_key, 6), position), (parts,), jnp.float32, smallest / len(shards), largest / len(shards))
        return jnp.repeat(jnp.exp(heights), dims[position] // parts).reshape((-1,) + (1,) * (len(dims) - position - 1))

    gain = one(*shards[0])
    for cut in shards[1:]:
        gain = gain * one(*cut)
    return gain


def noise(key, shape, width, most, shards=(), dtype=jnp.bfloat16):
    entries = jax.random.normal(key, shape, jnp.float32) * width
    if len(shards) > 0:
        entries = block_levels(key, shape, shards, -0.22, 0.18) * entries
    return jnp.clip(entries, min=-most, max=most).astype(dtype)


def setup_inputs(seed: int = 0) -> dict:
    key_of = jax.random.split(jax.random.key(seed), 6)
    return {
        "points": noise(key_of[0], (NPTS, D), 1.0, 6.0, ((0, 32),)),
        "weights": jnp.clip(jnp.exp(math.log(5.0) - 2.3025851 * jax.random.uniform(key_of[1], (NPTS,), jnp.float32) ** block_levels(key_of[1], (NPTS,), ((0, 32),), -0.2, 0.2)), 0.5, 5.0),
        "coverage": jnp.clip(-0.5 + 1.5 * jax.random.uniform(key_of[2], (NPTS,), jnp.float32) ** block_levels(key_of[2], (NPTS,), ((0, 32),), -0.2, 0.2), -0.5, 1.0),
        "candidates": noise(key_of[3], (NCAND, D), 1.0, 6.0, ((0, 16),)),
        "picks": set_ends(jax.random.randint(key_of[4], (NPICK,), 0, NCAND), jax.random.fold_in(key_of[4], 1), 0, NCAND - 1).astype(jnp.int32),
    }


def reference(points, weights, coverage, candidates, picks):
    scale = D ** -0.5
    total = points.shape[0]
    blocks = candidates.reshape(N_CAND, CAND_DEV, D)

    def block_gain(block):
        sims = jnp.dot(points, block.T, preferred_element_type=jnp.float32) * scale
        return jnp.sum(weights[:, None] * jnp.maximum(sims - coverage[:, None], 0.0), axis=0) / total

    gains = lax.map(block_gain, blocks).reshape(-1)
    top_gains = lax.top_k(gains, TOPK)[0]
    picked = jnp.take(candidates, picks.astype(jnp.int32), axis=0)
    picked_sims = jnp.dot(points, picked.T, preferred_element_type=jnp.float32) * scale
    new_coverage = jnp.maximum(coverage, jnp.max(picked_sims, axis=1))
    return gains, top_gains, new_coverage
```

```python
import functools

import jax
import jax.numpy as jnp
from jax import lax
from jax.experimental import pallas as pl
from jax.experimental.pallas import tpu as pltpu
from jax.sharding import PartitionSpec as P

TOPK = 64
LANES = 128
FAR = -1e30


def column_blocks(rows):
    turned = rows.T
    return [
        jnp.broadcast_to(turned[:, s : s + 1], (LANES, LANES)) for s in range(rows.shape[0])
    ]


def descending(values):
    n = values.shape[0]
    above = [jnp.zeros((8, LANES), jnp.float32) for _ in range(n)]
    for block in column_blocks(values):
        for r in range(n):
            larger = jnp.where(block > values[r : r + 1, :], 1.0, 0.0)
            above[r] = above[r] + larger.reshape(LANES // 8, 8, LANES).sum(axis=0)
    place = lax.broadcasted_iota(jnp.int32, (LANES, LANES), 0).astype(jnp.float32)
    best = jnp.full((LANES, LANES), jnp.inf, jnp.float32)
    for r in range(n):
        count = above[r].sum(axis=0, keepdims=True)
        best = jnp.minimum(best, jnp.where(count <= place, values[r : r + 1, :], jnp.inf))
    return best.T.min(axis=0, keepdims=True)


def scores_kernel(
    scale, total, n_pts, offset_ref, picks_ref, weights_ref, coverage_ref, points_hbm, cands_hbm,
    gains_ref, best_ref, points, cands, cover_cols, weight_cols, sems,
):
    chunks = points.shape[0] // 256
    parts = cands.shape[0] // 256

    def fetch(src, dst, i, sem):
        return pltpu.make_async_copy(
            src.at[pl.ds(i * 256, 256), :], dst.at[pl.ds(i * 256, 256), :], sem
        )

    point_copies = [fetch(points_hbm, points, i, sems.at[i]) for i in range(chunks)]
    cand_copies = [fetch(cands_hbm, cands, i, sems.at[chunks + i]) for i in range(parts)]
    for copy in [point_copies[0], *cand_copies, *point_copies[1:]]:
        copy.start()

    for s, block in enumerate(column_blocks(coverage_ref[...] * (1.0 / scale))):
        cover_cols[s * LANES : (s + 1) * LANES, :] = block
    for s, block in enumerate(column_blocks(weights_ref[...] * (scale / total))):
        weight_cols[s * LANES : (s + 1) * LANES, :] = block
    rows = cands.shape[0] // LANES
    mine = (
        offset_ref[0]
        + lax.broadcasted_iota(jnp.int32, (rows, LANES), 0) * LANES
        + lax.broadcasted_iota(jnp.int32, (rows, LANES), 1)
    )
    chosen = mine == picks_ref[0]
    for k in range(1, picks_ref.shape[0]):
        chosen = jnp.logical_or(chosen, mine == picks_ref[k])
    barred = jnp.where(chosen, 0.0, FAR)

    sums = [jnp.zeros((8, LANES), jnp.float32) for _ in range(rows)]
    for i in range(chunks):
        point_copies[i].wait()
        block = points[i * 256 : (i + 1) * 256, :]
        cover = cover_cols[i * 256 : (i + 1) * 256, :]
        weight = weight_cols[i * 256 : (i + 1) * 256, :]
        best = jnp.full((256, LANES), FAR, jnp.float32)
        for j in range(parts):
            if i == 0:
                cand_copies[j].wait()
            sims = lax.dot_general(
                block, cands[j * 256 : (j + 1) * 256, :], (((1,), (1,)), ((), ())),
                preferred_element_type=jnp.float32,
            )
            for h in range(2):
                r = 2 * j + h
                part = sims[:, h * LANES : (h + 1) * LANES]
                value = jnp.maximum(part - cover, 0.0) * weight
                sums[r] = sums[r] + value.reshape(32, 8, LANES).sum(axis=0)
                best = jnp.maximum(best, part + barred[r : r + 1, :])
        for h in range(2):
            turned = best[h * LANES : (h + 1) * LANES, :].T
            best_ref[0:1, (2 * i + h) * LANES : (2 * i + h + 1) * LANES] = (
                turned.max(axis=0, keepdims=True) * scale
            )
    gains = jnp.concatenate([s.sum(axis=0, keepdims=True) for s in sums], axis=0)
    gains_ref[...] = jnp.broadcast_to(gains[None], (n_pts, rows, LANES))


def gather_kernel(n_cand, partial_ref, best_ref, gains_ref, out_ref):
    gains = partial_ref[...].sum(axis=0)
    gains_ref[...] = gains
    top = descending(gains)
    for i in range(n_cand):
        out_ref[i, :, 0:LANES] = top
        out_ref[i, :, LANES:] = best_ref[...]


def final_kernel(all_ref, coverage_ref, gains_ref, gains_out, top_out, coverage_out):
    gains_out[...] = gains_ref[...]
    n = all_ref.shape[0]
    best = all_ref[0, :, LANES:]
    for i in range(1, n):
        best = jnp.maximum(best, all_ref[i, :, LANES:])
    coverage_out[...] = jnp.maximum(coverage_ref[...], best)
    even = jnp.concatenate([all_ref[i, :, 0:LANES] for i in range(0, n, 2)], axis=0)
    odd = jnp.concatenate([all_ref[i, :, 0:LANES] for i in range(1, n, 2)], axis=0)
    lane = lax.broadcasted_iota(jnp.int32, even.shape, 1)
    tops = jnp.where(lane < TOPK, even, pltpu.roll(odd, TOPK, 1))
    top_out[...] = descending(tops)[:, 0:TOPK]


def on_device(points, weights, coverage, candidates, picks):
    n_pts, n_cand = lax.axis_size("pts"), lax.axis_size("cand")
    local, width = points.shape
    cand_rows = candidates.shape[0]
    scale = width ** (-0.5)
    offset = (lax.axis_index("cand") * cand_rows).astype(jnp.int32).reshape(1)
    rows = cand_rows // LANES
    vmem = pl.BlockSpec(memory_space=pltpu.VMEM)
    smem = pl.BlockSpec(memory_space=pltpu.SMEM)
    hbm = pl.BlockSpec(memory_space=pltpu.HBM)
    f32 = jnp.float32

    partial, best = pl.pallas_call(
        functools.partial(scores_kernel, scale, float(local * n_pts), n_pts),
        out_shape=(
            jax.ShapeDtypeStruct((n_pts, rows, LANES), f32),
            jax.ShapeDtypeStruct((1, local), f32),
        ),
        in_specs=[smem, smem, vmem, vmem, hbm, hbm],
        out_specs=(vmem, vmem),
        scratch_shapes=[
            pltpu.VMEM(points.shape, points.dtype),
            pltpu.VMEM(candidates.shape, candidates.dtype),
            pltpu.VMEM((local, LANES), f32),
            pltpu.VMEM((local, LANES), f32),
            pltpu.SemaphoreType.DMA((local // 256 + cand_rows // 256,)),
        ],
        compiler_params=pltpu.CompilerParams(vmem_limit_bytes=24 * 1024 * 1024),
        cost_estimate=pl.CostEstimate(
            flops=2 * local * cand_rows * width, bytes_accessed=4 * 1024 * 1024, transcendentals=0
        ),
    )(
        offset,
        *(
            pltpu.with_memory_space_constraint(x, pltpu.HBM)
            for x in (
                picks, weights.reshape(-1, LANES), coverage.reshape(-1, LANES), points, candidates
            )
        ),
    )

    partial = lax.all_to_all(partial, "pts", split_axis=0, concat_axis=0, tiled=True)

    gains, message = pl.pallas_call(
        functools.partial(gather_kernel, n_cand),
        out_shape=(
            jax.ShapeDtypeStruct((rows, LANES), f32),
            jax.ShapeDtypeStruct((n_cand, 1, LANES + local), f32),
        ),
        in_specs=[vmem, vmem],
        out_specs=(vmem, vmem),
        compiler_params=pltpu.CompilerParams(vmem_limit_bytes=8 * 1024 * 1024),
    )(partial, best)

    message = lax.all_to_all(message, "cand", split_axis=0, concat_axis=0, tiled=True)

    gains, top_gains, new_coverage = pl.pallas_call(
        final_kernel,
        out_shape=(
            jax.ShapeDtypeStruct((rows, LANES), f32),
            jax.ShapeDtypeStruct((1, TOPK), f32),
            jax.ShapeDtypeStruct((1, local), f32),
        ),
        in_specs=[vmem, vmem, vmem],
        out_specs=(vmem, vmem, vmem),
        compiler_params=pltpu.CompilerParams(vmem_limit_bytes=8 * 1024 * 1024),
    )(message, coverage.reshape(1, -1), gains)
    return gains.reshape(-1), top_gains.reshape(-1), new_coverage.reshape(-1)


def solution(mesh):
    placed = (P("pts", None), P("pts"), P("pts"), P("cand", None), P())
    return jax.shard_map(
        on_device, mesh=mesh, in_specs=placed, out_specs=(P("cand"), P(), P("pts")), check_vma=False
    )
```

```python
import functools

import jax
import jax.numpy as jnp
from jax import lax
from jax.experimental import pallas as pl
from jax.experimental.pallas import tpu as pltpu
from jax.sharding import PartitionSpec as P

TOPK = 64
LANES = 128
FAR = -1e30


def column_blocks(rows):
    turned = rows.T
    return [
        jnp.broadcast_to(turned[:, s : s + 1], (LANES, LANES)) for s in range(rows.shape[0])
    ]


def descending(values):
    n = values.shape[0]
    above = [jnp.zeros((8, LANES), jnp.float32) for _ in range(n)]
    for block in column_blocks(values):
        for r in range(n):
            larger = jnp.where(block > values[r : r + 1, :], 1.0, 0.0)
            above[r] = above[r] + larger.reshape(LANES // 8, 8, LANES).sum(axis=0)
    place = lax.broadcasted_iota(jnp.int32, (LANES, LANES), 0).astype(jnp.float32)
    best = jnp.full((LANES, LANES), jnp.inf, jnp.float32)
    for r in range(n):
        count = above[r].sum(axis=0, keepdims=True)
        best = jnp.minimum(best, jnp.where(count <= place, values[r : r + 1, :], jnp.inf))
    return best.T.min(axis=0, keepdims=True)


def scores_kernel(
    scale, total, n_pts, picks_hbm, weights_hbm, coverage_hbm, points_hbm, cands_hbm,
    gains_ref, best_ref, points, cands, cover_cols, weight_cols, picks, weights, coverage, sems,
):
    operands = (
        (picks_hbm, picks), (weights_hbm, weights), (coverage_hbm, coverage),
        (points_hbm, points), (cands_hbm, cands),
    )
    copies = [
        pltpu.make_async_copy(src, dst, sems.at[i]) for i, (src, dst) in enumerate(operands)
    ]
    for copy in copies:
        copy.start()

    for copy in copies[:3]:
        copy.wait()
    for s, block in enumerate(column_blocks(coverage[...] * (1.0 / scale))):
        cover_cols[s * LANES : (s + 1) * LANES, :] = block
    for s, block in enumerate(column_blocks(weights[...] * (scale / total))):
        weight_cols[s * LANES : (s + 1) * LANES, :] = block
    local, rows = points.shape[0], cands.shape[0] // LANES
    mine = (
        lax.axis_index("cand") * cands.shape[0]
        + lax.broadcasted_iota(jnp.int32, (rows, LANES), 0) * LANES
        + lax.broadcasted_iota(jnp.int32, (rows, LANES), 1)
    )
    chosen = mine == picks[0]
    for k in range(1, picks.shape[0]):
        chosen = jnp.logical_or(chosen, mine == picks[k])
    barred = jnp.where(chosen, 0.0, FAR)

    for copy in copies[3:]:
        copy.wait()
    sums = []
    best = None
    for j in range(0, rows, 2):
        sims = lax.dot_general(
            points[...], cands[j * LANES : (j + 2) * LANES, :], (((1,), (1,)), ((), ())),
            preferred_element_type=jnp.float32,
        )
        for h in range(2):
            part = sims[:, h * LANES : (h + 1) * LANES]
            value = jnp.maximum(part - cover_cols[...], 0.0) * weight_cols[...]
            sums.append(value.reshape(local // 8, 8, LANES).sum(axis=0).sum(axis=0, keepdims=True))
            part = part + barred[j + h : j + h + 1, :]
            best = part if best is None else jnp.maximum(best, part)
    for r in range(0, local, LANES):
        turned = best[r : r + LANES, :].T
        best_ref[0:1, r : r + LANES] = turned.max(axis=0, keepdims=True) * scale
    gains_ref[...] = jnp.broadcast_to(jnp.concatenate(sums, axis=0)[None], (n_pts, rows, LANES))


def gather_kernel(n_cand, partial_ref, best_ref, gains_ref, out_ref):
    gains = partial_ref[...].sum(axis=0)
    gains_ref[...] = gains
    top = descending(gains)
    for i in range(n_cand):
        out_ref[i, :, 0:LANES] = top
        out_ref[i, :, LANES:] = best_ref[...]


def final_kernel(all_ref, coverage_ref, gains_ref, gains_out, top_out, coverage_out):
    gains_out[...] = gains_ref[...]
    n = all_ref.shape[0]
    best = all_ref[0, :, LANES:]
    for i in range(1, n):
        best = jnp.maximum(best, all_ref[i, :, LANES:])
    coverage_out[...] = jnp.maximum(coverage_ref[...], best)
    even = jnp.concatenate([all_ref[i, :, 0:LANES] for i in range(0, n, 2)], axis=0)
    odd = jnp.concatenate([all_ref[i, :, 0:LANES] for i in range(1, n, 2)], axis=0)
    lane = lax.broadcasted_iota(jnp.int32, even.shape, 1)
    tops = jnp.where(lane < TOPK, even, pltpu.roll(odd, TOPK, 1))
    top_out[...] = descending(tops)[:, 0:TOPK]


def on_device(points, weights, coverage, candidates, picks):
    n_pts, n_cand = lax.axis_size("pts"), lax.axis_size("cand")
    local, width = points.shape
    cand_rows = candidates.shape[0]
    scale = width ** (-0.5)
    rows = cand_rows // LANES
    vmem = pl.BlockSpec(memory_space=pltpu.VMEM)
    hbm = pl.BlockSpec(memory_space=pltpu.HBM)
    f32 = jnp.float32

    partial, best = pl.pallas_call(
        functools.partial(scores_kernel, scale, float(local * n_pts), n_pts),
        out_shape=(
            jax.ShapeDtypeStruct((n_pts, rows, LANES), f32),
            jax.ShapeDtypeStruct((1, local), f32),
        ),
        in_specs=[hbm] * 5,
        out_specs=(vmem, vmem),
        scratch_shapes=[
            pltpu.VMEM(points.shape, points.dtype),
            pltpu.VMEM(candidates.shape, candidates.dtype),
            pltpu.VMEM((local, LANES), f32),
            pltpu.VMEM((local, LANES), f32),
            pltpu.SMEM(picks.shape, picks.dtype),
            pltpu.VMEM((local // LANES, LANES), f32),
            pltpu.VMEM((local // LANES, LANES), f32),
            pltpu.SemaphoreType.DMA((5,)),
        ],
        compiler_params=pltpu.CompilerParams(vmem_limit_bytes=24 * 1024 * 1024),
        cost_estimate=pl.CostEstimate(
            flops=2 * local * cand_rows * width, bytes_accessed=4 * 1024 * 1024, transcendentals=0
        ),
    )(
        *(
            pltpu.with_memory_space_constraint(x, pltpu.HBM)
            for x in (
                picks, weights.reshape(-1, LANES), coverage.reshape(-1, LANES), points, candidates
            )
        ),
    )

    partial = lax.all_to_all(partial, "pts", split_axis=0, concat_axis=0, tiled=True)

    gains, message = pl.pallas_call(
        functools.partial(gather_kernel, n_cand),
        out_shape=(
            jax.ShapeDtypeStruct((rows, LANES), f32),
            jax.ShapeDtypeStruct((n_cand, 1, LANES + local), f32),
        ),
        in_specs=[vmem, vmem],
        out_specs=(vmem, vmem),
        compiler_params=pltpu.CompilerParams(vmem_limit_bytes=8 * 1024 * 1024),
    )(partial, best)

    message = lax.all_to_all(message, "cand", split_axis=0, concat_axis=0, tiled=True)

    gains, top_gains, new_coverage = pl.pallas_call(
        final_kernel,
        out_shape=(
            jax.ShapeDtypeStruct((rows, LANES), f32),
            jax.ShapeDtypeStruct((1, TOPK), f32),
            jax.ShapeDtypeStruct((1, local), f32),
        ),
        in_specs=[vmem, vmem, vmem],
        out_specs=(vmem, vmem, vmem),
        compiler_params=pltpu.CompilerParams(vmem_limit_bytes=8 * 1024 * 1024),
    )(message, coverage.reshape(1, -1), gains)
    return gains.reshape(-1), top_gains.reshape(-1), new_coverage.reshape(-1)


def solution(mesh):
    placed = (P("pts", None), P("pts"), P("pts"), P("cand", None), P())
    return jax.shard_map(
        on_device, mesh=mesh, in_specs=placed, out_specs=(P("cand"), P(), P("pts")), check_vma=False
    )
```

```python
import functools

import jax
import jax.numpy as jnp
from jax import lax
from jax.experimental import pallas as pl
from jax.experimental.pallas import tpu as pltpu
from jax.sharding import PartitionSpec as P

TOPK = 64
LANES = 128
FAR = -1e30
FIRST_PTS = 21
FIRST_CAND = 11


def column_blocks(rows):
    turned = rows.T
    return [
        jnp.broadcast_to(turned[:, s : s + 1], (LANES, LANES)) for s in range(rows.shape[0])
    ]


def descending(values):
    n = values.shape[0]
    above = [jnp.zeros((8, LANES), jnp.float32) for _ in range(n)]
    for block in column_blocks(values):
        for r in range(n):
            larger = jnp.where(block > values[r : r + 1, :], 1.0, 0.0)
            above[r] = above[r] + larger.reshape(LANES // 8, 8, LANES).sum(axis=0)
    place = lax.broadcasted_iota(jnp.int32, (LANES, LANES), 0).astype(jnp.float32)
    best = jnp.full((LANES, LANES), jnp.inf, jnp.float32)
    for r in range(n):
        count = above[r].sum(axis=0, keepdims=True)
        best = jnp.minimum(best, jnp.where(count <= place, values[r : r + 1, :], jnp.inf))
    return best.T.min(axis=0, keepdims=True)


def scores_kernel(
    scale, total, n_pts, picks_hbm, weights_hbm, coverage_hbm, points_hbm, cands_hbm,
    gains_ref, best_ref, points, cands, cover_cols, weight_cols, picks, weights, coverage, sems,
):
    operands = (
        (picks_hbm, picks), (weights_hbm, weights), (coverage_hbm, coverage),
        (points_hbm, points), (cands_hbm, cands),
    )
    copies = [
        pltpu.make_async_copy(src, dst, sems.at[i]) for i, (src, dst) in enumerate(operands)
    ]
    for copy in copies:
        copy.start()

    for copy in copies[:3]:
        copy.wait()
    for s, block in enumerate(column_blocks(coverage[...] * (1.0 / scale))):
        cover_cols[s * LANES : (s + 1) * LANES, :] = block
    for s, block in enumerate(column_blocks(weights[...] * (scale / total))):
        weight_cols[s * LANES : (s + 1) * LANES, :] = block
    local, rows = points.shape[0], cands.shape[0] // LANES
    mine = (
        lax.axis_index("cand") * cands.shape[0]
        + lax.broadcasted_iota(jnp.int32, (rows, LANES), 0) * LANES
        + lax.broadcasted_iota(jnp.int32, (rows, LANES), 1)
    )
    chosen = mine == picks[0]
    for k in range(1, picks.shape[0]):
        chosen = jnp.logical_or(chosen, mine == picks[k])
    barred = jnp.where(chosen, 0.0, FAR)

    for copy in copies[3:]:
        copy.wait()
    sums = []
    best = None
    for j in range(0, rows, 2):
        sims = lax.dot_general(
            points[...], cands[j * LANES : (j + 2) * LANES, :], (((1,), (1,)), ((), ())),
            preferred_element_type=jnp.float32,
        )
        for h in range(2):
            part = sims[:, h * LANES : (h + 1) * LANES]
            value = jnp.maximum(part - cover_cols[...], 0.0) * weight_cols[...]
            sums.append(value.reshape(local // 8, 8, LANES).sum(axis=0).sum(axis=0, keepdims=True))
            part = part + barred[j + h : j + h + 1, :]
            best = part if best is None else jnp.maximum(best, part)
    for r in range(0, local, LANES):
        turned = best[r : r + LANES, :].T
        best_ref[0:1, r : r + LANES] = turned.max(axis=0, keepdims=True) * scale
    gains_ref[...] = jnp.broadcast_to(jnp.concatenate(sums, axis=0)[None], (n_pts, rows, LANES))


def gather_kernel(n_cand, partial_ref, best_ref, gains_ref, out_ref):
    gains = partial_ref[...].sum(axis=0)
    gains_ref[...] = gains
    top = descending(gains)
    for i in range(n_cand):
        out_ref[i, :, 0:LANES] = top
        out_ref[i, :, LANES:] = best_ref[...]


def final_kernel(all_ref, coverage_ref, gains_ref, gains_out, top_out, coverage_out):
    gains_out[...] = gains_ref[...]
    n = all_ref.shape[0]
    best = all_ref[0, :, LANES:]
    for i in range(1, n):
        best = jnp.maximum(best, all_ref[i, :, LANES:])
    coverage_out[...] = jnp.maximum(coverage_ref[...], best)
    even = jnp.concatenate([all_ref[i, :, 0:LANES] for i in range(0, n, 2)], axis=0)
    odd = jnp.concatenate([all_ref[i, :, 0:LANES] for i in range(1, n, 2)], axis=0)
    lane = lax.broadcasted_iota(jnp.int32, even.shape, 1)
    tops = jnp.where(lane < TOPK, even, pltpu.roll(odd, TOPK, 1))
    top_out[...] = descending(tops)[:, 0:TOPK]


def exchanged(x, axis, first):
    n = lax.axis_size(axis)
    members = [[(first + i) % n for i in range(n)]]
    return lax.all_to_all(
        x, axis, split_axis=0, concat_axis=0, axis_index_groups=members, tiled=True
    )


def on_device(points, weights, coverage, candidates, picks):
    n_pts, n_cand = lax.axis_size("pts"), lax.axis_size("cand")
    local, width = points.shape
    cand_rows = candidates.shape[0]
    scale = width ** (-0.5)
    rows = cand_rows // LANES
    vmem = pl.BlockSpec(memory_space=pltpu.VMEM)
    hbm = pl.BlockSpec(memory_space=pltpu.HBM)
    f32 = jnp.float32

    partial, best = pl.pallas_call(
        functools.partial(scores_kernel, scale, float(local * n_pts), n_pts),
        out_shape=(
            jax.ShapeDtypeStruct((n_pts, rows, LANES), f32),
            jax.ShapeDtypeStruct((1, local), f32),
        ),
        in_specs=[hbm] * 5,
        out_specs=(vmem, vmem),
        scratch_shapes=[
            pltpu.VMEM(points.shape, points.dtype),
            pltpu.VMEM(candidates.shape, candidates.dtype),
            pltpu.VMEM((local, LANES), f32),
            pltpu.VMEM((local, LANES), f32),
            pltpu.SMEM(picks.shape, picks.dtype),
            pltpu.VMEM((local // LANES, LANES), f32),
            pltpu.VMEM((local // LANES, LANES), f32),
            pltpu.SemaphoreType.DMA((5,)),
        ],
        compiler_params=pltpu.CompilerParams(vmem_limit_bytes=24 * 1024 * 1024),
        cost_estimate=pl.CostEstimate(
            flops=2 * local * cand_rows * width, bytes_accessed=4 * 1024 * 1024, transcendentals=0
        ),
    )(
        *(
            pltpu.with_memory_space_constraint(x, pltpu.HBM)
            for x in (
                picks, weights.reshape(-1, LANES), coverage.reshape(-1, LANES), points, candidates
            )
        ),
    )

    partial = exchanged(partial, "pts", FIRST_PTS)

    gains, message = pl.pallas_call(
        functools.partial(gather_kernel, n_cand),
        out_shape=(
            jax.ShapeDtypeStruct((rows, LANES), f32),
            jax.ShapeDtypeStruct((n_cand, 1, LANES + local), f32),
        ),
        in_specs=[vmem, vmem],
        out_specs=(vmem, vmem),
        compiler_params=pltpu.CompilerParams(vmem_limit_bytes=8 * 1024 * 1024),
    )(partial, best)

    message = exchanged(message, "cand", FIRST_CAND)

    gains, top_gains, new_coverage = pl.pallas_call(
        final_kernel,
        out_shape=(
            jax.ShapeDtypeStruct((rows, LANES), f32),
            jax.ShapeDtypeStruct((1, TOPK), f32),
            jax.ShapeDtypeStruct((1, local), f32),
        ),
        in_specs=[vmem, vmem, vmem],
        out_specs=(vmem, vmem, vmem),
        compiler_params=pltpu.CompilerParams(vmem_limit_bytes=8 * 1024 * 1024),
    )(message, coverage.reshape(1, -1), gains)
    return gains.reshape(-1), top_gains.reshape(-1), new_coverage.reshape(-1)


def solution(mesh):
    placed = (P("pts", None), P("pts"), P("pts"), P("cand", None), P())
    return jax.shard_map(
        on_device, mesh=mesh, in_specs=placed, out_specs=(P("cand"), P(), P("pts")), check_vma=False
    )
```

```python
import functools

import jax
import jax.numpy as jnp
from jax import lax
from jax.experimental import pallas as pl
from jax.experimental.pallas import tpu as pltpu
from jax.sharding import PartitionSpec as P

TOPK = 64
LANES = 128
FAR = -1e30
FIRST_PTS = 21
FIRST_CAND = 11


def column_blocks(rows):
    turned = rows.T
    return [
        jnp.broadcast_to(turned[:, s : s + 1], (LANES, LANES)) for s in range(rows.shape[0])
    ]


def ranked(values, place):
    n = values.shape[0]
    above = [jnp.zeros((8, LANES), jnp.float32) for _ in range(n)]
    for block in column_blocks(values):
        for r in range(n):
            larger = jnp.where(block > values[r : r + 1, :], 1.0, 0.0)
            above[r] = above[r] + larger.reshape(LANES // 8, 8, LANES).sum(axis=0)
    best = jnp.full((LANES, LANES), jnp.inf, jnp.float32)
    for r in range(n):
        count = above[r].sum(axis=0, keepdims=True)
        best = jnp.minimum(best, jnp.where(count <= place, values[r : r + 1, :], jnp.inf))
    return best.T.min(axis=0, keepdims=True)


def scores_kernel(
    scale, total, n_pts, picks_hbm, weights_hbm, coverage_hbm, points_hbm, cands_hbm,
    gains_ref, best_ref, points, cands, cover_cols, weight_cols, picks, weights, coverage, sems,
):
    operands = (
        (picks_hbm, picks), (weights_hbm, weights), (coverage_hbm, coverage),
        (points_hbm, points), (cands_hbm, cands),
    )
    copies = [
        pltpu.make_async_copy(src, dst, sems.at[i]) for i, (src, dst) in enumerate(operands)
    ]
    for copy in copies:
        copy.start()

    for copy in copies[:3]:
        copy.wait()
    for s, block in enumerate(column_blocks(coverage[...] * (1.0 / scale))):
        cover_cols[s * LANES : (s + 1) * LANES, :] = block
    for s, block in enumerate(column_blocks(weights[...] * (scale / total))):
        weight_cols[s * LANES : (s + 1) * LANES, :] = block
    local, rows = points.shape[0], cands.shape[0] // LANES
    mine = (
        lax.axis_index("cand") * cands.shape[0]
        + lax.broadcasted_iota(jnp.int32, (rows, LANES), 0) * LANES
        + lax.broadcasted_iota(jnp.int32, (rows, LANES), 1)
    )
    chosen = mine == picks[0]
    for k in range(1, picks.shape[0]):
        chosen = jnp.logical_or(chosen, mine == picks[k])
    barred = jnp.where(chosen, 0.0, FAR)

    for copy in copies[3:]:
        copy.wait()
    sums = [jnp.zeros((8, LANES), jnp.float32) for _ in range(rows)]
    half = local // 2
    best = [None, None]
    for j in range(0, rows, 2):
        last = j == rows - 2
        for first, size in ((0, half), (half, half)) if last else ((0, local),):
            span = slice(first, first + size)
            sims = lax.dot_general(
                points[span, :], cands[j * LANES : (j + 2) * LANES, :], (((1,), (1,)), ((), ())),
                preferred_element_type=jnp.float32,
            )
            masked = None
            for h in range(2):
                part = sims[:, h * LANES : (h + 1) * LANES]
                value = jnp.maximum(part - cover_cols[span, :], 0.0) * weight_cols[span, :]
                sums[j + h] = sums[j + h] + value.reshape(size // 8, 8, LANES).sum(axis=0)
                part = part + barred[j + h : j + h + 1, :]
                masked = part if masked is None else jnp.maximum(masked, part)
            for q in range(first // half, (first + size) // half):
                piece = masked[q * half - first : (q + 1) * half - first, :]
                best[q] = piece if best[q] is None else jnp.maximum(best[q], piece)
                for r in range(0, half if last else 0, LANES):
                    turned = best[q][r : r + LANES, :].T
                    best_ref[0:1, q * half + r : q * half + r + LANES] = (
                        turned.max(axis=0, keepdims=True) * scale
                    )
    sums = [s.sum(axis=0, keepdims=True) for s in sums]
    gains_ref[...] = jnp.broadcast_to(jnp.concatenate(sums, axis=0)[None], (n_pts, rows, LANES))


def gather_kernel(n_cand, partial_ref, best_ref, gains_ref, out_ref):
    gains = partial_ref[...].sum(axis=0)
    gains_ref[...] = gains
    row = lax.broadcasted_iota(jnp.int32, (LANES, LANES), 0)
    falling = lax.axis_index("cand") % 2 == 0
    top = ranked(gains, jnp.where(falling, row, TOPK - 1 - row).astype(jnp.float32))
    for i in range(n_cand):
        out_ref[i, :, 0:LANES] = top
        out_ref[i, :, LANES:] = best_ref[...]


def final_kernel(all_ref, coverage_ref, gains_ref, gains_out, top_out, coverage_out):
    gains_out[...] = gains_ref[...]
    n = all_ref.shape[0]
    best = all_ref[0, :, LANES:]
    for i in range(1, n):
        best = jnp.maximum(best, all_ref[i, :, LANES:])
    coverage_out[...] = jnp.maximum(coverage_ref[...], best)
    pairs = [
        jnp.maximum(all_ref[i, :, 0:LANES], all_ref[i + 1, :, 0:LANES]) for i in range(0, n, 2)
    ]
    left, right = (jnp.concatenate(half, axis=0) for half in (pairs[0::2], pairs[1::2]))
    lane = lax.broadcasted_iota(jnp.int32, left.shape, 1)
    tops = jnp.where(lane < TOPK, left, pltpu.roll(right, TOPK, 1))
    place = lax.broadcasted_iota(jnp.int32, (LANES, LANES), 0).astype(jnp.float32)
    top_out[...] = ranked(tops, place)[:, 0:TOPK]


def exchanged(x, axis, first):
    n = lax.axis_size(axis)
    members = [[(first + i) % n for i in range(n)]]
    return lax.all_to_all(
        x, axis, split_axis=0, concat_axis=0, axis_index_groups=members, tiled=True
    )


def on_device(points, weights, coverage, candidates, picks):
    n_pts, n_cand = lax.axis_size("pts"), lax.axis_size("cand")
    local, width = points.shape
    cand_rows = candidates.shape[0]
    scale = width ** (-0.5)
    rows = cand_rows // LANES
    vmem = pl.BlockSpec(memory_space=pltpu.VMEM)
    hbm = pl.BlockSpec(memory_space=pltpu.HBM)
    f32 = jnp.float32

    partial, best = pl.pallas_call(
        functools.partial(scores_kernel, scale, float(local * n_pts), n_pts),
        out_shape=(
            jax.ShapeDtypeStruct((n_pts, rows, LANES), f32),
            jax.ShapeDtypeStruct((1, local), f32),
        ),
        in_specs=[hbm] * 5,
        out_specs=(vmem, vmem),
        scratch_shapes=[
            pltpu.VMEM(points.shape, points.dtype),
            pltpu.VMEM(candidates.shape, candidates.dtype),
            pltpu.VMEM((local, LANES), f32),
            pltpu.VMEM((local, LANES), f32),
            pltpu.SMEM(picks.shape, picks.dtype),
            pltpu.VMEM((local // LANES, LANES), f32),
            pltpu.VMEM((local // LANES, LANES), f32),
            pltpu.SemaphoreType.DMA((5,)),
        ],
        compiler_params=pltpu.CompilerParams(vmem_limit_bytes=24 * 1024 * 1024),
        cost_estimate=pl.CostEstimate(
            flops=2 * local * cand_rows * width, bytes_accessed=4 * 1024 * 1024, transcendentals=0
        ),
    )(
        *(
            pltpu.with_memory_space_constraint(x, pltpu.HBM)
            for x in (
                picks, weights.reshape(-1, LANES), coverage.reshape(-1, LANES), points, candidates
            )
        ),
    )

    partial = exchanged(partial, "pts", FIRST_PTS)

    gains, message = pl.pallas_call(
        functools.partial(gather_kernel, n_cand),
        out_shape=(
            jax.ShapeDtypeStruct((rows, LANES), f32),
            jax.ShapeDtypeStruct((n_cand, 1, LANES + local), f32),
        ),
        in_specs=[vmem, vmem],
        out_specs=(vmem, vmem),
        compiler_params=pltpu.CompilerParams(vmem_limit_bytes=8 * 1024 * 1024),
    )(partial, best)

    message = exchanged(message, "cand", FIRST_CAND)

    gains, top_gains, new_coverage = pl.pallas_call(
        final_kernel,
        out_shape=(
            jax.ShapeDtypeStruct((rows, LANES), f32),
            jax.ShapeDtypeStruct((1, TOPK), f32),
            jax.ShapeDtypeStruct((1, local), f32),
        ),
        in_specs=[vmem, vmem, vmem],
        out_specs=(vmem, vmem, vmem),
        compiler_params=pltpu.CompilerParams(vmem_limit_bytes=8 * 1024 * 1024),
    )(message, coverage.reshape(1, -1), gains)
    return gains.reshape(-1), top_gains.reshape(-1), new_coverage.reshape(-1)


def solution(mesh):
    placed = (P("pts", None), P("pts"), P("pts"), P("cand", None), P())
    return jax.shard_map(
        on_device, mesh=mesh, in_specs=placed, out_specs=(P("cand"), P(), P("pts")), check_vma=False
    )
```

```python
import functools

import jax
import jax.numpy as jnp
from jax import lax
from jax.experimental import pallas as pl
from jax.experimental.pallas import tpu as pltpu
from jax.sharding import PartitionSpec as P

TOPK = 64
LANES = 128
FAR = -1e30
FIRST_PTS = 21
FIRST_CAND = 11


def column_blocks(rows):
    turned = rows.T
    return [
        jnp.broadcast_to(turned[:, s : s + 1], (LANES, LANES)) for s in range(rows.shape[0])
    ]


NETWORKS = {
    4: ((0, 1), (2, 3), (0, 2), (1, 3), (1, 2)),
    8: (
        (0, 1), (2, 3), (4, 5), (6, 7), (0, 2), (1, 3), (4, 6), (5, 7), (1, 2), (5, 6),
        (0, 4), (1, 5), (2, 6), (3, 7), (2, 4), (3, 5), (1, 2), (3, 4), (5, 6),
    ),
}


def lanes_sorted(values):
    rows = [values[r : r + 1, :] for r in range(values.shape[0])]
    for a, b in NETWORKS[len(rows)]:
        rows[a], rows[b] = jnp.maximum(rows[a], rows[b]), jnp.minimum(rows[a], rows[b])
    return rows


def count_above(rows, block):
    *rows, least = rows
    if len(rows) == 3:
        high = rows[1] > block
        low = jnp.where(high, rows[2], rows[0]) > block
        count = jnp.where(high, 2.0, 0.0) + jnp.where(low, 1.0, 0.0)
    else:
        high = rows[3] > block
        middle = jnp.where(high, rows[5], rows[1]) > block
        upper, lower = jnp.where(high, rows[6], rows[2]), jnp.where(high, rows[4], rows[0])
        low = jnp.where(middle, upper, lower) > block
        count = (
            jnp.where(high, 4.0, 0.0) + jnp.where(middle, 2.0, 0.0) + jnp.where(low, 1.0, 0.0)
        )
    return count + jnp.where(least > block, 1.0, 0.0)


def ranked(values, place):
    rows = lanes_sorted(values)
    best = jnp.full((8, LANES), jnp.inf, jnp.float32)
    for block in column_blocks(jnp.concatenate(rows, axis=0)):
        above = count_above(rows, block).sum(axis=1, keepdims=True)
        found = jnp.where(above <= place, block, jnp.inf)
        best = jnp.minimum(best, found.reshape(LANES // 8, 8, LANES).min(axis=0))
    return best.min(axis=0, keepdims=True)


def scores_kernel(
    scale, total, n_pts, picks_hbm, weights_hbm, coverage_hbm, points_hbm, cands_hbm,
    gains_ref, best_ref, points, cands, cover_cols, weight_cols, picks, weights, coverage, sems,
):
    operands = (
        (picks_hbm, picks), (weights_hbm, weights), (coverage_hbm, coverage),
        (points_hbm, points), (cands_hbm, cands),
    )
    copies = [
        pltpu.make_async_copy(src, dst, sems.at[i]) for i, (src, dst) in enumerate(operands)
    ]
    for copy in copies:
        copy.start()

    for copy in copies[:3]:
        copy.wait()
    for s, block in enumerate(column_blocks(coverage[...] * (1.0 / scale))):
        cover_cols[s * LANES : (s + 1) * LANES, :] = block
    for s, block in enumerate(column_blocks(weights[...] * (scale / total))):
        weight_cols[s * LANES : (s + 1) * LANES, :] = block
    local, rows = points.shape[0], cands.shape[0] // LANES
    mine = (
        lax.axis_index("cand") * cands.shape[0]
        + lax.broadcasted_iota(jnp.int32, (rows, LANES), 0) * LANES
        + lax.broadcasted_iota(jnp.int32, (rows, LANES), 1)
    )
    chosen = mine == picks[0]
    for k in range(1, picks.shape[0]):
        chosen = jnp.logical_or(chosen, mine == picks[k])
    barred = jnp.where(chosen, 0.0, FAR)

    for copy in copies[3:]:
        copy.wait()
    sums = [jnp.zeros((8, LANES), jnp.float32) for _ in range(rows)]
    half = local // 2
    best = [None, None]
    for j in range(0, rows, 2):
        last = j == rows - 2
        for first, size in ((0, half), (half, half)) if last else ((0, local),):
            span = slice(first, first + size)
            sims = lax.dot_general(
                points[span, :], cands[j * LANES : (j + 2) * LANES, :], (((1,), (1,)), ((), ())),
                preferred_element_type=jnp.float32,
            )
            masked = None
            for h in range(2):
                part = sims[:, h * LANES : (h + 1) * LANES]
                value = jnp.maximum(part - cover_cols[span, :], 0.0) * weight_cols[span, :]
                sums[j + h] = sums[j + h] + value.reshape(size // 8, 8, LANES).sum(axis=0)
                part = part + barred[j + h : j + h + 1, :]
                masked = part if masked is None else jnp.maximum(masked, part)
            for q in range(first // half, (first + size) // half):
                piece = masked[q * half - first : (q + 1) * half - first, :]
                best[q] = piece if best[q] is None else jnp.maximum(best[q], piece)
                for r in range(0, half if last else 0, LANES):
                    turned = best[q][r : r + LANES, :].T
                    best_ref[0:1, q * half + r : q * half + r + LANES] = (
                        turned.max(axis=0, keepdims=True) * scale
                    )
    sums = [s.sum(axis=0, keepdims=True) for s in sums]
    gains_ref[...] = jnp.broadcast_to(jnp.concatenate(sums, axis=0)[None], (n_pts, rows, LANES))


def gather_kernel(n_cand, partial_ref, best_ref, gains_ref, out_ref):
    gains = partial_ref[...].sum(axis=0)
    gains_ref[...] = gains
    lane = lax.broadcasted_iota(jnp.int32, (1, LANES), 1)
    falling = lax.axis_index("cand") % 2 == 0
    top = ranked(gains, jnp.where(falling, lane, TOPK - 1 - lane).astype(jnp.float32))
    for i in range(n_cand):
        out_ref[i, :, 0:LANES] = top
        out_ref[i, :, LANES:] = best_ref[...]


def final_kernel(all_ref, coverage_ref, gains_ref, gains_out, top_out, coverage_out):
    gains_out[...] = gains_ref[...]
    n = all_ref.shape[0]
    best = all_ref[0, :, LANES:]
    for i in range(1, n):
        best = jnp.maximum(best, all_ref[i, :, LANES:])
    coverage_out[...] = jnp.maximum(coverage_ref[...], best)
    pairs = [
        jnp.maximum(all_ref[i, :, 0:LANES], all_ref[i + 1, :, 0:LANES]) for i in range(0, n, 2)
    ]
    left, right = (jnp.concatenate(half, axis=0) for half in (pairs[0::2], pairs[1::2]))
    lane = lax.broadcasted_iota(jnp.int32, left.shape, 1)
    tops = jnp.where(lane < TOPK, left, pltpu.roll(right, TOPK, 1))
    place = lax.broadcasted_iota(jnp.int32, (1, LANES), 1).astype(jnp.float32)
    top_out[...] = ranked(tops, place)[:, 0:TOPK]


def exchanged(x, axis, first):
    n = lax.axis_size(axis)
    members = [[(first + i) % n for i in range(n)]]
    return lax.all_to_all(
        x, axis, split_axis=0, concat_axis=0, axis_index_groups=members, tiled=True
    )


def on_device(points, weights, coverage, candidates, picks):
    n_pts, n_cand = lax.axis_size("pts"), lax.axis_size("cand")
    local, width = points.shape
    cand_rows = candidates.shape[0]
    scale = width ** (-0.5)
    rows = cand_rows // LANES
    vmem = pl.BlockSpec(memory_space=pltpu.VMEM)
    hbm = pl.BlockSpec(memory_space=pltpu.HBM)
    f32 = jnp.float32

    partial, best = pl.pallas_call(
        functools.partial(scores_kernel, scale, float(local * n_pts), n_pts),
        out_shape=(
            jax.ShapeDtypeStruct((n_pts, rows, LANES), f32),
            jax.ShapeDtypeStruct((1, local), f32),
        ),
        in_specs=[hbm] * 5,
        out_specs=(vmem, vmem),
        scratch_shapes=[
            pltpu.VMEM(points.shape, points.dtype),
            pltpu.VMEM(candidates.shape, candidates.dtype),
            pltpu.VMEM((local, LANES), f32),
            pltpu.VMEM((local, LANES), f32),
            pltpu.SMEM(picks.shape, picks.dtype),
            pltpu.VMEM((local // LANES, LANES), f32),
            pltpu.VMEM((local // LANES, LANES), f32),
            pltpu.SemaphoreType.DMA((5,)),
        ],
        compiler_params=pltpu.CompilerParams(vmem_limit_bytes=24 * 1024 * 1024),
        cost_estimate=pl.CostEstimate(
            flops=2 * local * cand_rows * width, bytes_accessed=4 * 1024 * 1024, transcendentals=0
        ),
    )(
        *(
            pltpu.with_memory_space_constraint(x, pltpu.HBM)
            for x in (
                picks, weights.reshape(-1, LANES), coverage.reshape(-1, LANES), points, candidates
            )
        ),
    )

    partial = exchanged(partial, "pts", FIRST_PTS)

    gains, message = pl.pallas_call(
        functools.partial(gather_kernel, n_cand),
        out_shape=(
            jax.ShapeDtypeStruct((rows, LANES), f32),
            jax.ShapeDtypeStruct((n_cand, 1, LANES + local), f32),
        ),
        in_specs=[vmem, vmem],
        out_specs=(vmem, vmem),
        compiler_params=pltpu.CompilerParams(vmem_limit_bytes=8 * 1024 * 1024),
    )(partial, best)

    message = exchanged(message, "cand", FIRST_CAND)

    gains, top_gains, new_coverage = pl.pallas_call(
        final_kernel,
        out_shape=(
            jax.ShapeDtypeStruct((rows, LANES), f32),
            jax.ShapeDtypeStruct((1, TOPK), f32),
            jax.ShapeDtypeStruct((1, local), f32),
        ),
        in_specs=[vmem, vmem, vmem],
        out_specs=(vmem, vmem, vmem),
        compiler_params=pltpu.CompilerParams(vmem_limit_bytes=8 * 1024 * 1024),
    )(message, coverage.reshape(1, -1), gains)
    return gains.reshape(-1), top_gains.reshape(-1), new_coverage.reshape(-1)


def solution(mesh):
    placed = (P("pts", None), P("pts"), P("pts"), P("cand", None), P())
    return jax.shard_map(
        on_device, mesh=mesh, in_specs=placed, out_specs=(P("cand"), P(), P("pts")), check_vma=False
    )
```

```python
import functools

import jax
import jax.numpy as jnp
from jax import lax
from jax.experimental import pallas as pl
from jax.experimental.pallas import tpu as pltpu
from jax.sharding import PartitionSpec as P

TOPK = 64
LANES = 128
FAR = -1e30
FIRST_PTS = 21
FIRST_CAND = 11


def column_blocks(rows):
    turned = rows.T
    return [
        jnp.broadcast_to(turned[:, s : s + 1], (LANES, LANES)) for s in range(rows.shape[0])
    ]


NETWORKS = {
    4: ((0, 1), (2, 3), (0, 2), (1, 3), (1, 2)),
    8: (
        (0, 1), (2, 3), (4, 5), (6, 7), (0, 2), (1, 3), (4, 6), (5, 7), (1, 2), (5, 6),
        (0, 4), (1, 5), (2, 6), (3, 7), (2, 4), (3, 5), (1, 2), (3, 4), (5, 6),
    ),
}


def lanes_sorted(values):
    rows = [values[r : r + 1, :] for r in range(values.shape[0])]
    for a, b in NETWORKS[len(rows)]:
        rows[a], rows[b] = jnp.maximum(rows[a], rows[b]), jnp.minimum(rows[a], rows[b])
    return rows


def count_above(rows, block):
    *rows, least = rows
    if len(rows) == 3:
        high = rows[1] > block
        low = jnp.where(high, rows[2], rows[0]) > block
        count = jnp.where(high, 2.0, 0.0) + jnp.where(low, 1.0, 0.0)
    else:
        high = rows[3] > block
        middle = jnp.where(high, rows[5], rows[1]) > block
        upper, lower = jnp.where(high, rows[6], rows[2]), jnp.where(high, rows[4], rows[0])
        low = jnp.where(middle, upper, lower) > block
        count = (
            jnp.where(high, 4.0, 0.0) + jnp.where(middle, 2.0, 0.0) + jnp.where(low, 1.0, 0.0)
        )
    return count + jnp.where(least > block, 1.0, 0.0)


def ranked(values, place):
    rows = lanes_sorted(values)
    best = jnp.full((8, LANES), jnp.inf, jnp.float32)
    for block in column_blocks(jnp.concatenate(rows, axis=0)):
        above = count_above(rows, block).sum(axis=1, keepdims=True)
        found = jnp.where(above <= place, block, jnp.inf)
        best = jnp.minimum(best, found.reshape(LANES // 8, 8, LANES).min(axis=0))
    return best.min(axis=0, keepdims=True)


def scores_kernel(
    scale, total, n_pts, picks_hbm, weights_hbm, coverage_hbm, points_hbm, cands_hbm,
    gains_ref, best_ref, points, cands, cover_cols, weight_cols, picks, weights, coverage, sems,
):
    step = points.shape[0] // 2, cands.shape[0] // 2
    operands = [(picks_hbm, picks), (weights_hbm, weights), (coverage_hbm, coverage)]
    for i in range(2):
        for (src, dst), size in zip(((points_hbm, points), (cands_hbm, cands)), step, strict=True):
            piece = slice(i * size, (i + 1) * size)
            operands.append((src.at[piece, :], dst.at[piece, :]))
    copies = [
        pltpu.make_async_copy(src, dst, sems.at[i]) for i, (src, dst) in enumerate(operands)
    ]
    for copy in copies:
        copy.start()

    for copy in copies[:3]:
        copy.wait()
    for s, block in enumerate(column_blocks(coverage[...] * (1.0 / scale))):
        cover_cols[s * LANES : (s + 1) * LANES, :] = block
    for s, block in enumerate(column_blocks(weights[...] * (scale / total))):
        weight_cols[s * LANES : (s + 1) * LANES, :] = block
    local, rows = points.shape[0], cands.shape[0] // LANES
    mine = (
        lax.axis_index("cand") * cands.shape[0]
        + lax.broadcasted_iota(jnp.int32, (rows, LANES), 0) * LANES
        + lax.broadcasted_iota(jnp.int32, (rows, LANES), 1)
    )
    chosen = mine == picks[0]
    for k in range(1, picks.shape[0]):
        chosen = jnp.logical_or(chosen, mine == picks[k])
    barred = jnp.where(chosen, 0.0, FAR)

    for copy in copies[3:]:
        copy.wait()
    sums = [jnp.zeros((8, LANES), jnp.float32) for _ in range(rows)]
    half = local // 2
    best = [None, None]
    for j in range(0, rows, 2):
        last = j == rows - 2
        for first, size in ((0, half), (half, half)) if last else ((0, local),):
            span = slice(first, first + size)
            sims = lax.dot_general(
                points[span, :], cands[j * LANES : (j + 2) * LANES, :], (((1,), (1,)), ((), ())),
                preferred_element_type=jnp.float32,
            )
            masked = None
            for h in range(2):
                part = sims[:, h * LANES : (h + 1) * LANES]
                value = jnp.maximum(part - cover_cols[span, :], 0.0) * weight_cols[span, :]
                sums[j + h] = sums[j + h] + value.reshape(size // 8, 8, LANES).sum(axis=0)
                part = part + barred[j + h : j + h + 1, :]
                masked = part if masked is None else jnp.maximum(masked, part)
            for q in range(first // half, (first + size) // half):
                piece = masked[q * half - first : (q + 1) * half - first, :]
                best[q] = piece if best[q] is None else jnp.maximum(best[q], piece)
                for r in range(0, half if last else 0, LANES):
                    turned = best[q][r : r + LANES, :].T
                    best_ref[0:1, q * half + r : q * half + r + LANES] = (
                        turned.max(axis=0, keepdims=True) * scale
                    )
    sums = [s.sum(axis=0, keepdims=True) for s in sums]
    gains_ref[...] = jnp.broadcast_to(jnp.concatenate(sums, axis=0)[None], (n_pts, rows, LANES))


def gather_kernel(n_cand, partial_ref, best_ref, gains_ref, out_ref):
    gains = partial_ref[...].sum(axis=0)
    gains_ref[...] = gains
    lane = lax.broadcasted_iota(jnp.int32, (1, LANES), 1)
    falling = lax.axis_index("cand") % 2 == 0
    top = ranked(gains, jnp.where(falling, lane, TOPK - 1 - lane).astype(jnp.float32))
    for i in range(n_cand):
        out_ref[i, :, 0:LANES] = top
        out_ref[i, :, LANES:] = best_ref[...]


def final_kernel(all_ref, coverage_ref, gains_ref, gains_out, top_out, coverage_out):
    gains_out[...] = gains_ref[...]
    n = all_ref.shape[0]
    best = all_ref[0, :, LANES:]
    for i in range(1, n):
        best = jnp.maximum(best, all_ref[i, :, LANES:])
    coverage_out[...] = jnp.maximum(coverage_ref[...], best)
    pairs = [
        jnp.maximum(all_ref[i, :, 0:LANES], all_ref[i + 1, :, 0:LANES]) for i in range(0, n, 2)
    ]
    left, right = (jnp.concatenate(half, axis=0) for half in (pairs[0::2], pairs[1::2]))
    lane = lax.broadcasted_iota(jnp.int32, left.shape, 1)
    tops = jnp.where(lane < TOPK, left, pltpu.roll(right, TOPK, 1))
    place = lax.broadcasted_iota(jnp.int32, (1, LANES), 1).astype(jnp.float32)
    top_out[...] = ranked(tops, place)[:, 0:TOPK]


def exchanged(x, axis, first):
    n = lax.axis_size(axis)
    members = [[(first + i) % n for i in range(n)]]
    return lax.all_to_all(
        x, axis, split_axis=0, concat_axis=0, axis_index_groups=members, tiled=True
    )


def on_device(points, weights, coverage, candidates, picks):
    n_pts, n_cand = lax.axis_size("pts"), lax.axis_size("cand")
    local, width = points.shape
    cand_rows = candidates.shape[0]
    scale = width ** (-0.5)
    rows = cand_rows // LANES
    vmem = pl.BlockSpec(memory_space=pltpu.VMEM)
    hbm = pl.BlockSpec(memory_space=pltpu.HBM)
    f32 = jnp.float32

    partial, best = pl.pallas_call(
        functools.partial(scores_kernel, scale, float(local * n_pts), n_pts),
        out_shape=(
            jax.ShapeDtypeStruct((n_pts, rows, LANES), f32),
            jax.ShapeDtypeStruct((1, local), f32),
        ),
        in_specs=[hbm] * 5,
        out_specs=(vmem, vmem),
        scratch_shapes=[
            pltpu.VMEM(points.shape, points.dtype),
            pltpu.VMEM(candidates.shape, candidates.dtype),
            pltpu.VMEM((local, LANES), f32),
            pltpu.VMEM((local, LANES), f32),
            pltpu.SMEM(picks.shape, picks.dtype),
            pltpu.VMEM((local // LANES, LANES), f32),
            pltpu.VMEM((local // LANES, LANES), f32),
            pltpu.SemaphoreType.DMA((7,)),
        ],
        compiler_params=pltpu.CompilerParams(
            vmem_limit_bytes=24 * 1024 * 1024,
        ),
        cost_estimate=pl.CostEstimate(
            flops=2 * local * cand_rows * width, bytes_accessed=4 * 1024 * 1024, transcendentals=0
        ),
    )(
        *(
            pltpu.with_memory_space_constraint(x, pltpu.HBM)
            for x in (
                picks, weights.reshape(-1, LANES), coverage.reshape(-1, LANES), points, candidates
            )
        ),
    )

    partial = exchanged(partial, "pts", FIRST_PTS)

    gains, message = pl.pallas_call(
        functools.partial(gather_kernel, n_cand),
        out_shape=(
            jax.ShapeDtypeStruct((rows, LANES), f32),
            jax.ShapeDtypeStruct((n_cand, 1, LANES + local), f32),
        ),
        in_specs=[vmem, vmem],
        out_specs=(vmem, vmem),
        compiler_params=pltpu.CompilerParams(vmem_limit_bytes=8 * 1024 * 1024),
    )(partial, best)

    message = exchanged(message, "cand", FIRST_CAND)

    gains, top_gains, new_coverage = pl.pallas_call(
        final_kernel,
        out_shape=(
            jax.ShapeDtypeStruct((rows, LANES), f32),
            jax.ShapeDtypeStruct((1, TOPK), f32),
            jax.ShapeDtypeStruct((1, local), f32),
        ),
        in_specs=[vmem, vmem, vmem],
        out_specs=(vmem, vmem, vmem),
        compiler_params=pltpu.CompilerParams(vmem_limit_bytes=8 * 1024 * 1024),
    )(message, coverage.reshape(1, -1), gains)
    return gains.reshape(-1), top_gains.reshape(-1), new_coverage.reshape(-1)


def solution(mesh):
    placed = (P("pts", None), P("pts"), P("pts"), P("cand", None), P())
    return jax.shard_map(
        on_device, mesh=mesh, in_specs=placed, out_specs=(P("cand"), P(), P("pts")), check_vma=False
    )
```
